8 devices in a mesh: dp: 4 (over z, y, x), tp: 2 (over core).
Axes of the slice: x: 2, y: 2, z: 1, core: 2. Of those that a mesh axis runs over, the one named last changes fastest.
Arguments:
- x_teach: bfloat16 [16, 256, 1024], P('dp', 'tp')
- x_stud: bfloat16 [16, 256, 768], P(('dp', 'tp'))
- w_up_t: bfloat16 [8, 1024, 4096], P(None, None, 'tp')
- w_down_t: bfloat16 [8, 4096, 1024], P(None, 'tp')
- gain_t: float32 [8, 1024], replicated
- head_t: bfloat16 [1024, 50304], P(None, 'tp')
- w_up_s: bfloat16 [1, 768, 3072], replicated
- w_down_s: bfloat16 [1, 3072, 768], replicated
- gain_s: float32 [1, 768], replicated
- proj_s: bfloat16 [1, 768, 1024], replicated
- head_s: bfloat16 [768, 50304], replicated
Outputs:
- output 1: float32 [], replicated
- output 2: float32 [1, 768, 3072], replicated
- output 3: float32 [1, 3072, 768], replicated
- output 4: float32 [1, 768], replicated
- output 5: float32 [1, 768, 1024], replicated
- output 6: float32 [768, 50304], replicated
All inputs are finite; a program needn't handle non-finite values.
Results may differ from the reference program's by a relative error of at most 0.0168161.
Values are sent between devices in bfloat16 or wider.
A program may use at most 1.5 GiB of HBM per device.

```python
import jax
import jax.numpy as jnp
from jax import lax

BATCH = 16
SEQ_LEN = 256
D_TEACH = 1024
D_STUD = 768
VOCAB_SIZE = 50304
FEAT_LAYERS = 1
TEACH_LAYERS = 8
NORM_EPS = 1e-6


def setup_inputs(seed: int = 0) -> dict:
    rng_keys = jax.random.split(jax.random.key(seed), 11)
    ff_teach = 4 * D_TEACH
    ff_stud = 4 * D_STUD

    def normal_bf16(rng_key, arr_shape, std_scale):
        return (jax.random.normal(rng_key, arr_shape, jnp.float32) * std_scale).astype(jnp.bfloat16)

    return {
        'x_teach': normal_bf16(rng_keys[0], (BATCH, SEQ_LEN, D_TEACH), 1.0),
        'x_stud': normal_bf16(rng_keys[1], (BATCH, SEQ_LEN, D_STUD), 1.0),
        'w_up_t': normal_bf16(rng_keys[2], (TEACH_LAYERS, D_TEACH, ff_teach), D_TEACH ** -0.5),
        'w_down_t': normal_bf16(rng_keys[3], (TEACH_LAYERS, ff_teach, D_TEACH), ff_teach ** -0.5),
        'gain_t': jax.random.uniform(rng_keys[4], (TEACH_LAYERS, D_TEACH), jnp.float32, 0.5, 1.5),
        'head_t': normal_bf16(rng_keys[5], (D_TEACH, VOCAB_SIZE), D_TEACH ** -0.5),
        'w_up_s': normal_bf16(rng_keys[6], (FEAT_LAYERS, D_STUD, ff_stud), D_STUD ** -0.5),
        'w_down_s': normal_bf16(rng_keys[7], (FEAT_LAYERS, ff_stud, D_STUD), ff_stud ** -0.5),
        'gain_s': jax.random.uniform(rng_keys[8], (FEAT_LAYERS, D_STUD), jnp.float32, 0.5, 1.5),
        'proj_s': normal_bf16(rng_keys[9], (FEAT_LAYERS, D_STUD, D_TEACH), D_STUD ** -0.5),
        'head_s': normal_bf16(rng_keys[10], (D_STUD, VOCAB_SIZE), D_STUD ** -0.5),
    }


def rms_norm(values):
    vals32 = values.astype(jnp.float32)
    return vals32 * lax.rsqrt(jnp.mean(vals32 * vals32, axis=-1, keepdims=True) + NORM_EPS)


def as_bf16(values):
    return values.astype(jnp.bfloat16).astype(jnp.float32)


def gelu_tanh(values):
    return jax.nn.gelu(values, approximate=True)


def teacher_tokens(teach_blk, w_up_t, w_down_t, gain_t, head_t):
    per_feat = TEACH_LAYERS // FEAT_LAYERS
    up_groups = w_up_t.reshape(FEAT_LAYERS, per_feat, D_TEACH, 4 * D_TEACH)
    down_groups = w_down_t.reshape(FEAT_LAYERS, per_feat, 4 * D_TEACH, D_TEACH)
    gain_groups = gain_t.reshape(FEAT_LAYERS, per_feat, D_TEACH)

    def one_layer(hidden, layer_w):
        w_up, w_down, gain_row = layer_w
        normed = (rms_norm(hidden) * gain_row).astype(jnp.bfloat16)
        hidden_act = gelu_tanh(jnp.dot(normed, w_up, preferred_element_type=jnp.float32)).astype(jnp.bfloat16)
        layer_out = jnp.dot(hidden_act, w_down, preferred_element_type=jnp.float32).astype(jnp.bfloat16)
        return hidden + layer_out, None

    def one_feature(hidden, group_w):
        hidden, _ = lax.scan(one_layer, hidden, group_w)
        return hidden, hidden

    hidden, features = lax.scan(one_feature, teach_blk, (up_groups, down_groups, gain_groups))
    teach_logits = jnp.dot(rms_norm(hidden).astype(jnp.bfloat16), head_t, preferred_element_type=jnp.float32)
    return features, teach_logits


def student_loss(params, stud_blk, features, teach_logits, feat_coef, kl_coef):
    w_up, w_down, gains, proj, head_w = params

    def one_block(residual, layer_w):
        up_j, down_j, gain_j, proj_j, feat_j = layer_w
        normed = as_bf16(rms_norm(residual) * gain_j)
        hidden_act = as_bf16(gelu_tanh(jnp.dot(normed, up_j, preferred_element_type=jnp.float32)))
        residual = residual + jnp.dot(hidden_act, down_j, preferred_element_type=jnp.float32)
        proj_in = as_bf16(rms_norm(residual))
        feat_err = jnp.dot(proj_in, proj_j, preferred_element_type=jnp.float32) - feat_j.astype(jnp.float32)
        return residual, jnp.sum(feat_err * feat_err)

    residual, err_sums = lax.scan(one_block, stud_blk.astype(jnp.float32), (w_up, w_down, gains, proj, features))
    stud_logits = jnp.dot(as_bf16(rms_norm(residual)), head_w, preferred_element_type=jnp.float32)
    log_teach = jax.nn.log_softmax(teach_logits, axis=-1)
    log_stud = jax.nn.log_softmax(stud_logits, axis=-1)
    kl_sum = jnp.sum(jnp.exp(log_teach) * (log_teach - log_stud))
    return feat_coef * jnp.sum(err_sums) + kl_coef * kl_sum


def reference(x_teach, x_stud, w_up_t, w_down_t, gain_t, head_t, w_up_s, w_down_s, gain_s, proj_s, head_s):
    block_len = 128
    n_tokens = BATCH * SEQ_LEN
    n_blocks = n_tokens // block_len
    teach_blocks = x_teach.reshape(n_blocks, block_len, D_TEACH)
    stud_blocks = x_stud.reshape(n_blocks, block_len, D_STUD)
    params = (w_up_s.astype(jnp.float32), w_down_s.astype(jnp.float32), gain_s.astype(jnp.float32),
              proj_s.astype(jnp.float32), head_s.astype(jnp.float32))
    feat_coef = 1.0 / (FEAT_LAYERS * n_tokens * D_TEACH)
    kl_coef = 1.0 / n_tokens
    loss_and_grad = jax.value_and_grad(student_loss)

    def one_block(scan_carry, token_blks):
        loss_acc, grad_acc = scan_carry
        teach_blk, stud_blk = token_blks
        features, teach_logits = teacher_tokens(teach_blk, w_up_t, w_down_t, gain_t, head_t)
        loss_val, grad_vals = loss_and_grad(params, stud_blk, features, teach_logits, feat_coef, kl_coef)
        return (loss_acc + loss_val, jax.tree.map(jnp.add, grad_acc, grad_vals)), None

    start_carry = (jnp.zeros((), jnp.float32), jax.tree.map(jnp.zeros_like, params))
    (total_loss, grad_vals), _ = lax.scan(one_block, start_carry, (teach_blocks, stud_blocks))
    grad_up, grad_down, grad_gain, grad_proj, grad_head = grad_vals
    return (total_loss, grad_up, grad_down, grad_gain, grad_proj, grad_head)
```

```python
import functools

import jax
import jax.numpy as jnp
from jax import lax
from jax.experimental import pallas as pl
from jax.experimental.pallas import tpu as pltpu
from jax.sharding import PartitionSpec as P


NORM_EPS = 1e-6
NEG = -3.0e38
BLK = 512
N_BLK = 50
N_OWN = 7
N_SHARED = 4 * N_OWN
OWN_SPLIT = (4, 3)
RED_SPLIT = (11, 11)
VMEM_LIMIT = 60 * 1024 * 1024


def rms_parts(values):
    vals32 = values.astype(jnp.float32)
    inv_rms = lax.rsqrt(jnp.mean(vals32 * vals32, axis=-1, keepdims=True) + NORM_EPS)
    return vals32 * inv_rms, inv_rms


def rms_back(normed, inv_rms, grad_out):
    return inv_rms * (grad_out - normed * jnp.mean(grad_out * normed, axis=-1, keepdims=True))


def gelu_tanh(values):
    return jax.nn.gelu(values, approximate=True)


def gelu_back(pre_act, grad_out):
    return jax.vjp(gelu_tanh, pre_act)[1](grad_out)[0]


def mat_mul(subscripts, lhs_arr, rhs_arr):
    return jnp.einsum(subscripts, lhs_arr, rhs_arr, preferred_element_type=jnp.float32)


def dot_f32(lhs, rhs):
    return jnp.dot(lhs, rhs, preferred_element_type=jnp.float32)


def dot_rows(lhs, rhs):
    return lax.dot_general(lhs, rhs, (((1,), (1,)), ((), ())), preferred_element_type=jnp.float32)


def valid_cols(core, blk, half_cols):
    cols = blk * BLK + lax.broadcasted_iota(jnp.int32, (1, BLK), 1)
    return (cols >= 64 * core) & (cols < half_cols + 64 * core)


def stats_kernel(half_cols, meta, ht, rs, wt, ws, zt_out, zs_out, st_out, mt, st, at, ms, ss):
    blk = pl.program_id(0)
    valid = valid_cols(meta[0], blk, half_cols)

    @pl.when(blk == 0)
    def _():
        mt[...] = jnp.full_like(mt, NEG)
        ms[...] = jnp.full_like(ms, NEG)
        st[...] = jnp.zeros_like(st)
        at[...] = jnp.zeros_like(at)
        ss[...] = jnp.zeros_like(ss)

    rows_all = ht.shape[0]
    step = 512
    for row in range(0, rows_all, step):
        rows = pl.ds(row, step)
        zt = jnp.where(valid, dot_rows(ht[rows, :], wt[...]), NEG)
        zs = jnp.where(valid, dot_f32(rs[rows, :], ws[...]), NEG)
        zt_out[rows, :] = zt
        zs_out[rows, :] = zs
        parts_t = [zt[:, j:j + 128] for j in range(0, BLK, 128)]
        parts_s = [zs[:, j:j + 128] for j in range(0, BLK, 128)]
        m_old = mt[rows, :]
        m_new = functools.reduce(jnp.maximum, parts_t, m_old)
        corr = jnp.exp(m_old - m_new)
        exps = [jnp.exp(p - m_new) for p in parts_t]
        st[rows, :] = st[rows, :] * corr + sum(exps)
        at[rows, :] = at[rows, :] * corr + sum(e * (p - q) for e, p, q in zip(exps, parts_t, parts_s))
        mt[rows, :] = m_new
        m_old = ms[rows, :]
        m_new = functools.reduce(jnp.maximum, parts_s, m_old)
        corr = jnp.exp(m_old - m_new)
        ss[rows, :] = ss[rows, :] * corr + sum(jnp.exp(p - m_new) for p in parts_s)
        ms[rows, :] = m_new

    @pl.when(blk == pl.num_programs(0) - 1)
    def _():
        top_t = jnp.max(mt[...], axis=-1, keepdims=True)
        scale = jnp.exp(mt[...] - top_t)
        sum_t = jnp.sum(st[...] * scale, axis=-1, keepdims=True)
        sum_a = jnp.sum(at[...] * scale, axis=-1, keepdims=True)
        top_s = jnp.max(ms[...], axis=-1, keepdims=True)
        sum_s = jnp.sum(ss[...] * jnp.exp(ms[...] - top_s), axis=-1, keepdims=True)
        lane = lax.broadcasted_iota(jnp.int32, st_out.shape, 1)
        res = jnp.where(lane == 0, top_t, jnp.where(lane == 1, sum_t, sum_a))
        res = jnp.where(lane == 3, top_s, jnp.where(lane == 4, sum_s, res))
        st_out[...] = res


def head_stats(meta, ht, rs, hts, head_s, half_cols):
    rows, d_t = ht.shape
    d_s = rs.shape[1]
    cols = N_BLK * BLK
    grid_spec = pltpu.PrefetchScalarGridSpec(
        num_scalar_prefetch=1,
        grid=(N_BLK,),
        in_specs=[
            pl.BlockSpec((rows, d_t), lambda k, m: (0, 0), pipeline_mode=pl.Buffered(1)),
            pl.BlockSpec((rows, d_s), lambda k, m: (0, 0), pipeline_mode=pl.Buffered(1)),
            pl.BlockSpec((BLK, d_t), lambda k, m: (k, 0)),
            pl.BlockSpec((d_s, BLK), lambda k, m: (0, k + (N_BLK - 1) * m[0])),
        ],
        out_specs=[
            pl.BlockSpec((rows, BLK), lambda k, m: (0, k)),
            pl.BlockSpec((rows, BLK), lambda k, m: (0, k)),
            pl.BlockSpec((rows, 128), lambda k, m: (0, 0)),
        ],
        scratch_shapes=[pltpu.VMEM((rows, 128), jnp.float32)] * 5,
    )
    return pl.pallas_call(
        functools.partial(stats_kernel, half_cols),
        grid_spec=grid_spec,
        out_shape=[
            jax.ShapeDtypeStruct((rows, cols), jnp.float32),
            jax.ShapeDtypeStruct((rows, cols), jnp.float32),
            jax.ShapeDtypeStruct((rows, 128), jnp.float32),
        ],
        compiler_params=pltpu.CompilerParams(dimension_semantics=("arbitrary",), vmem_limit_bytes=VMEM_LIMIT),
        cost_estimate=pl.CostEstimate(
            flops=2 * rows * cols * (d_t + d_s), bytes_accessed=cols * (2 * (d_t + d_s) + 8 * rows),
            transcendentals=2 * rows * cols),
        name="head_stats",
    )(meta, ht, rs, hts, head_s)


def logit_grad(zt, zs, lse_t, lse_s, coef):
    return (coef * (jnp.exp(zs - lse_s) - jnp.exp(zt - lse_t))).astype(jnp.bfloat16)


def grad_kernel(half_cols, coef, meta, ht, rs, rst, lt, ls, wt, ws, zt_own, zs_own, out):
    own = meta[1]
    valid = valid_cols(meta[0], meta[2] + pl.program_id(0), half_cols)
    lg = logit_grad(zt_own[...], zs_own[...], lt[own], ls[own], coef)
    out[...] = dot_f32(rst[own], lg)
    for other in range(1, 4):
        grp = lax.rem(own + other, 4)
        zt = jnp.where(valid, dot_rows(ht[grp], wt[...]), NEG)
        zs = jnp.where(valid, dot_f32(rs[grp], ws[...]), NEG)
        out[...] += dot_f32(rst[grp], logit_grad(zt, zs, lt[grp], ls[grp], coef))


def head_grad_blocks(n_blocks, meta, ht_all, rs_all, rst_all, lse_t, lse_s, hts, head_s, zt, zs, half_cols, coef):
    groups, rows, d_t = ht_all.shape
    d_s = rs_all.shape[2]

    def whole(shape):
        return pl.BlockSpec(shape, lambda i, m: (0,) * len(shape), pipeline_mode=pl.Buffered(1))

    grid_spec = pltpu.PrefetchScalarGridSpec(
        num_scalar_prefetch=1,
        grid=(n_blocks,),
        in_specs=[
            whole((groups, rows, d_t)),
            whole((groups, rows, d_s)),
            whole((groups, d_s, rows)),
            whole((groups, rows, 1)),
            whole((groups, rows, 1)),
            pl.BlockSpec((BLK, d_t), lambda i, m: (m[2] + i, 0)),
            pl.BlockSpec((d_s, BLK), lambda i, m: (0, m[2] + i + (N_BLK - 1) * m[0])),
            pl.BlockSpec((rows, BLK), lambda i, m: (0, m[2] + i)),
            pl.BlockSpec((rows, BLK), lambda i, m: (0, m[2] + i)),
        ],
        out_specs=pl.BlockSpec((d_s, BLK), lambda i, m: (0, i)),
    )
    cols = n_blocks * BLK
    return pl.pallas_call(
        functools.partial(grad_kernel, half_cols, coef),
        grid_spec=grid_spec,
        out_shape=jax.ShapeDtypeStruct((d_s, cols), jnp.float32),
        compiler_params=pltpu.CompilerParams(dimension_semantics=("arbitrary",), vmem_limit_bytes=VMEM_LIMIT),
        cost_estimate=pl.CostEstimate(
            flops=2 * rows * cols * (3 * d_t + 7 * d_s), bytes_accessed=cols * (2 * d_t + 6 * d_s + 8 * rows),
            transcendentals=8 * rows * cols),
        name="head_grad",
    )(meta, ht_all, rs_all, rst_all, lse_t, lse_s, hts, head_s, zt, zs)


def input_grad_kernel(coef, meta, lt, ls, zt, zs, ws, out):
    blk = pl.program_id(0)
    last = pl.num_programs(0) - 1

    @pl.when(blk == 0)
    def _():
        out[...] = jnp.zeros_like(out)

    @pl.when(blk < last)
    def _():
        lg = logit_grad(zt[...], zs[...], lt[...], ls[...], coef)
        out[...] += dot_rows(lg, ws[...])

    @pl.when(blk == last)
    def _():
        lg = logit_grad(zt[:, :128], zs[:, :128], lt[...], ls[...], coef)
        out[...] += dot_rows(lg, ws[:, :128])


def head_input_grad(meta, lse_t, lse_s, zt, zs, head_s, coef):
    rows = zt.shape[0]
    d_s = head_s.shape[0]
    cols = N_BLK * BLK
    grid_spec = pltpu.PrefetchScalarGridSpec(
        num_scalar_prefetch=1,
        grid=(N_BLK,),
        in_specs=[
            pl.BlockSpec((rows, 1), lambda k, m: (0, 0)),
            pl.BlockSpec((rows, 1), lambda k, m: (0, 0)),
            pl.BlockSpec((rows, BLK), lambda k, m: (0, k)),
            pl.BlockSpec((rows, BLK), lambda k, m: (0, k)),
            pl.BlockSpec((d_s, BLK), lambda k, m: (0, k + (N_BLK - 1) * m[0])),
        ],
        out_specs=pl.BlockSpec((rows, d_s), lambda k, m: (0, 0)),
    )
    return pl.pallas_call(
        functools.partial(input_grad_kernel, coef),
        grid_spec=grid_spec,
        out_shape=jax.ShapeDtypeStruct((rows, d_s), jnp.float32),
        compiler_params=pltpu.CompilerParams(dimension_semantics=("arbitrary",), vmem_limit_bytes=VMEM_LIMIT),
        cost_estimate=pl.CostEstimate(
            flops=4 * rows * cols * d_s, bytes_accessed=cols * (2 * d_s + 8 * rows), transcendentals=2 * rows * cols),
        name="head_input_grad",
    )(meta, lse_t, lse_s, zt, zs, head_s)


def block_pieces():
    shared = []
    for part, n_blocks in enumerate(OWN_SPLIT):
        for j in range(n_blocks):
            shared.append((part, j))
    pieces = {}
    for k in range(N_SHARED):
        part, j = shared[k % N_OWN]
        pieces[k] = (part, k // N_OWN, j * BLK)
    k = N_SHARED
    for part, n_blocks in enumerate(RED_SPLIT):
        for j in range(n_blocks):
            pieces[k] = (len(OWN_SPLIT) + part, None, j * BLK)
            k += 1
    return pieces


def piece_view(refs, piece, extra, width):
    part, lead, col = piece
    ref = refs[part]
    if lead is None:
        return ref.at[:, pl.ds(col + extra, width)]
    return ref.at[lead, :, pl.ds(col + extra, width)]


def assemble_kernel(n_arr, n_buf, meta, *refs):
    own, partner = refs[:n_arr], refs[n_arr:2 * n_arr]
    out, bufs, seam_a, seam_b, in_sem, out_sem, seam_sem = refs[2 * n_arr:]
    core = meta[0]
    pieces = block_pieces()
    seam_col = (N_BLK - 1) * BLK
    jobs = [(0, pieces[k], 0, k * BLK, BLK) for k in range(N_BLK - 1)]
    jobs.append((1, pieces[0], 128, seam_col + 128, BLK - 128))
    jobs += [(1, pieces[k], 0, seam_col + k * BLK, BLK) for k in range(1, N_BLK - 1)]
    jobs.append((1, pieces[N_BLK - 1], 0, seam_col + (N_BLK - 1) * BLK, 128))

    def fetch(half, piece, extra, width, dst, sem):
        @pl.when(core == half)
        def _():
            pltpu.make_async_copy(piece_view(own, piece, extra, width), dst, sem).start()

        @pl.when(core != half)
        def _():
            pltpu.make_async_copy(piece_view(partner, piece, extra, width), dst, sem).start()

    fetch(0, pieces[N_BLK - 1], 0, 128, seam_a, seam_sem.at[0])
    fetch(1, pieces[0], 0, 128, seam_b, seam_sem.at[1])

    def buf_of(i):
        return bufs.at[i % n_buf, :, pl.ds(0, jobs[i][4])]

    def start_in(i):
        half, piece, extra, _, width = jobs[i]
        fetch(half, piece, extra, width, buf_of(i), in_sem.at[i % n_buf])

    def out_copy(i):
        return pltpu.make_async_copy(buf_of(i), out.at[:, pl.ds(jobs[i][3], jobs[i][4])], out_sem.at[i % n_buf])

    def finish_in(i):
        pltpu.make_async_copy(buf_of(i), buf_of(i), in_sem.at[i % n_buf]).wait()
        out_copy(i).start()

    lag = n_buf // 2
    for i in range(len(jobs) + lag):
        if i < len(jobs):
            if i >= n_buf:
                out_copy(i - n_buf).wait()
            start_in(i)
        if i >= lag:
            finish_in(i - lag)
    pltpu.make_async_copy(seam_a, seam_a, seam_sem.at[0]).wait()
    pltpu.make_async_copy(seam_b, seam_b, seam_sem.at[1]).wait()
    seam_a[...] += seam_b[...]
    seam = pltpu.make_async_copy(seam_a, out.at[:, pl.ds(seam_col, 128)], seam_sem.at[0])
    seam.start()
    for i in range(len(jobs) - n_buf, len(jobs)):
        out_copy(i).wait()
    seam.wait()


def assemble(meta, own, partner, vocab):
    d_s = own[0].shape[-2]
    n_buf = 8
    any_spec = pl.BlockSpec(memory_space=pl.ANY)
    return pl.pallas_call(
        functools.partial(assemble_kernel, len(own), n_buf),
        in_specs=[pl.BlockSpec(memory_space=pltpu.SMEM)] + [any_spec] * (2 * len(own)),
        out_specs=any_spec,
        out_shape=jax.ShapeDtypeStruct((d_s, vocab), jnp.float32),
        scratch_shapes=[
            pltpu.VMEM((n_buf, d_s, BLK), jnp.float32),
            pltpu.VMEM((d_s, 128), jnp.float32),
            pltpu.VMEM((d_s, 128), jnp.float32),
            pltpu.SemaphoreType.DMA((n_buf,)),
            pltpu.SemaphoreType.DMA((n_buf,)),
            pltpu.SemaphoreType.DMA((2,)),
        ],
        compiler_params=pltpu.CompilerParams(vmem_limit_bytes=VMEM_LIMIT),
        cost_estimate=pl.CostEstimate(flops=d_s * vocab * 100, bytes_accessed=8 * d_s * vocab, transcendentals=0),
        name="assemble",
    )(meta, *own, *partner)


def after(value, *earlier):
    return lax.optimization_barrier((value, *earlier))[0]


def solution(mesh):
    dp_size = mesh.shape['dp']
    tp_size = mesh.shape['tp']
    swap = [(0, 1), (1, 0)]

    def local_step(x_teach, x_stud, w_up_t, w_down_t, gain_t, head_t, w_up_s, w_down_s, gain_s, proj_s, head_s):
        dp_idx = lax.axis_index('dp')
        core = lax.axis_index('tp')
        n_seq, seq_len, d_s = x_stud.shape
        d_t = x_teach.shape[-1]
        local_tok = n_seq * seq_len
        group_tok = local_tok * tp_size
        n_tokens = group_tok * dp_size
        half_cols = head_t.shape[1]
        vocab = head_s.shape[1]
        feat_coef = 1.0 / (n_tokens * d_t)
        kl_coef = 1.0 / n_tokens
        w_up, w_down, gain, proj = w_up_s[0], w_down_s[0], gain_s[0], proj_s[0]
        both = ('dp', 'tp')

        x_all = lax.all_gather(x_stud.reshape(local_tok, d_s), both, axis=0, tiled=True)
        norm_all, _ = rms_parts(x_all)
        n_all = (norm_all * gain).astype(jnp.bfloat16)

        norm_cur, _ = rms_parts(x_stud.reshape(local_tok, d_s))
        normed = (norm_cur * gain).astype(jnp.bfloat16)
        hidden_s = gelu_tanh(mat_mul('sd,df->sf', normed, w_up)).astype(jnp.bfloat16)
        residual = x_stud.reshape(local_tok, d_s).astype(jnp.float32) + mat_mul('sf,fd->sd', hidden_s, w_down)
        norm_next, inv_next = rms_parts(residual)
        proj_in = norm_next.astype(jnp.bfloat16)
        proj_out = mat_mul('sd,de->se', proj_in, proj)
        rs_flat = lax.all_gather(proj_in, both, axis=0, tiled=True)
        rs_all = rs_flat.reshape(dp_size, group_tok, d_s)
        rst_all = jnp.swapaxes(rs_all, 1, 2)
        rs_grp = lax.dynamic_index_in_dim(rs_all, dp_idx, 0, keepdims=False)

        padded = jnp.pad(head_t.T, ((64, N_BLK * BLK - half_cols), (0, 0)))
        hts = lax.dynamic_slice_in_dim(padded, 64 - 64 * core, N_BLK * BLK, axis=0)

        f_half = w_up.shape[1] // tp_size
        up_half = lax.dynamic_slice_in_dim(w_up, core * f_half, f_half, axis=1)
        down_half = lax.dynamic_slice_in_dim(w_down, core * f_half, f_half, axis=0)
        pre_half = mat_mul('sd,df->sf', n_all, up_half)
        act_half = gelu_tanh(pre_half).astype(jnp.bfloat16)

        hidden = x_teach
        for layer_idx in range(w_up_t.shape[0]):
            t_in = (rms_parts(hidden)[0] * gain_t[layer_idx]).astype(jnp.bfloat16)
            gathered = lax.all_gather(t_in, 'tp', axis=1, tiled=True)
            hidden_act = gelu_tanh(mat_mul('bsd,df->bsf', gathered, w_up_t[layer_idx])).astype(jnp.bfloat16)
            partial_out = mat_mul('bsf,fd->bsd', hidden_act, w_down_t[layer_idx])
            layer_out = lax.psum_scatter(partial_out, 'tp', scatter_dimension=1, tiled=True)
            hidden = hidden + layer_out.astype(jnp.bfloat16)
        feature = lax.all_to_all(hidden, 'tp', 0, 1, tiled=True)
        final_norm = rms_parts(hidden)[0].astype(jnp.bfloat16)
        ht_grp = lax.all_gather(final_norm, 'tp', axis=1, tiled=True).reshape(group_tok, d_t)
        ht_all = lax.all_gather(ht_grp, 'dp')

        meta0 = jnp.stack([core, dp_idx, jnp.int32(0)]).astype(jnp.int32)
        zt, zs, stats = head_stats(meta0, ht_grp, rs_grp, hts, head_s, half_cols)
        stats_all = lax.all_gather(stats[:, :8].T, both).reshape(dp_size, tp_size, 8, group_tok)
        top_t, sum_t, sum_a, top_s, sum_s = [stats_all[:, :, j, :] for j in range(5)]
        max_t = jnp.max(top_t, axis=1)
        max_s = jnp.max(top_s, axis=1)
        scale_t = jnp.exp(top_t - max_t[:, None])
        all_t = jnp.sum(sum_t * scale_t, axis=1)
        all_a = jnp.sum(sum_a * scale_t, axis=1)
        all_s = jnp.sum(sum_s * jnp.exp(top_s - max_s[:, None]), axis=1)
        lse_t = max_t + jnp.log(all_t)
        lse_s = max_s + jnp.log(all_s)
        kl_total = jnp.sum(all_a / all_t - lse_t + lse_s)
        lse_t = lse_t[..., None]
        lse_s = lse_s[..., None]

        def blocks(base, count, lse):
            meta = jnp.stack([core, dp_idx, base]).astype(jnp.int32)
            return head_grad_blocks(count, meta, ht_all, rs_all, rst_all, lse, lse_s, hts, head_s, zt, zs,
                                    half_cols, kl_coef)

        own_parts = []
        base, lse_o = dp_idx * N_OWN, lse_t
        for count in OWN_SPLIT:
            own_parts.append(blocks(base, count, lse_o))
            base = base + count
            lse_o = after(lse_t, own_parts[-1])
        shared = []
        for part in own_parts:
            shared.append(lax.all_gather(part, 'dp'))

        lse_own_t = lax.dynamic_index_in_dim(lse_o, dp_idx, 0, keepdims=False)
        lse_own_s = lax.dynamic_index_in_dim(lse_s, dp_idx, 0, keepdims=False)
        full_in_grad = head_input_grad(meta0, lse_own_t, lse_own_s, zt, zs, head_s, kl_coef)
        give = lax.dynamic_slice_in_dim(full_in_grad, (1 - core) * local_tok, local_tok, axis=0)
        keep = lax.dynamic_slice_in_dim(full_in_grad, core * local_tok, local_tok, axis=0)
        head_in_grad = keep + lax.ppermute(give, 'tp', swap)

        feat_err = proj_out - feature.reshape(local_tok, d_t)
        err_total = jnp.sum(feat_err * feat_err)
        err_grad = (2.0 * feat_coef * feat_err).astype(jnp.bfloat16)
        out_grad = mat_mul('se,de->sd', err_grad, proj)
        resid_grad = rms_back(norm_next, inv_next, out_grad + head_in_grad)
        resid_all = lax.all_gather(resid_grad.astype(jnp.bfloat16), both, axis=0, tiled=True)
        err_all = lax.all_gather(err_grad, both, axis=0, tiled=True)

        lse_r = after(lse_t, full_in_grad)
        redundant = []
        base = jnp.int32(N_SHARED)
        for count in RED_SPLIT:
            redundant.append(blocks(base, count, lse_r))
            base = base + count
            lse_r = after(lse_t, redundant[-1])
        own = shared + redundant
        partner = []
        for part in own:
            partner.append(lax.ppermute(part, 'tp', swap))

        resid_all = after(resid_all, redundant[-1])
        act_grad = mat_mul('sd,fd->sf', resid_all, down_half)
        pre_grad = gelu_back(pre_half, act_grad).astype(jnp.bfloat16)
        up_part = mat_mul('sd,sf->df', n_all, pre_grad)
        down_part = mat_mul('sf,sd->fd', act_half, resid_all)
        e_half = d_t // tp_size
        proj_part = mat_mul('sd,se->de', rs_flat, lax.dynamic_slice_in_dim(err_all, core * e_half, e_half, axis=1))
        pre_own = lax.dynamic_slice_in_dim(pre_grad, dp_idx * group_tok, group_tok, axis=0)
        norm_own = lax.dynamic_slice_in_dim(norm_all, dp_idx * group_tok, group_tok, axis=0)
        gain_part = jnp.sum(mat_mul('sf,df->sd', pre_own, up_half) * norm_own, axis=0)

        grad_up = lax.all_gather(up_part, 'tp', axis=1, tiled=True)[None]
        grad_down = lax.all_gather(down_part, 'tp', axis=0, tiled=True)[None]
        grad_proj = lax.all_gather(proj_part, 'tp', axis=1, tiled=True)[None]
        grad_gain, err_sum = lax.psum((gain_part, err_total), both)
        loss = feat_coef * err_sum + kl_coef * kl_total
        head_grad = assemble(meta0, own, partner, vocab)
        return loss, grad_up, grad_down, grad_gain[None], grad_proj, head_grad

    in_specs = (P('dp', 'tp', None), P(('dp', 'tp'), None, None), P(None, None, 'tp'), P(None, 'tp', None),
                P(), P(None, 'tp'), P(), P(), P(), P(), P())
    out_specs = (P(), P(), P(), P(), P(), P())

    return jax.shard_map(local_step, mesh=mesh, in_specs=in_specs, out_specs=out_specs, check_vma=False)
```

```python
import functools

import jax
import jax.numpy as jnp
from jax import lax
from jax.experimental import pallas as pl
from jax.experimental.pallas import tpu as pltpu
from jax.sharding import PartitionSpec as P


NORM_EPS = 1e-6
NEG = -3.0e38
BLK = 512
PIECE = 64
N_PIECE = BLK // PIECE
N_BLK = 50
N_OWN = 7
N_SHARED = 4 * N_OWN
OWN_SPLIT = (4, 3)
RED_SPLIT = (11, 11)
VMEM_LIMIT = 60 * 1024 * 1024


def rms_parts(values):
    vals32 = values.astype(jnp.float32)
    inv_rms = lax.rsqrt(jnp.mean(vals32 * vals32, axis=-1, keepdims=True) + NORM_EPS)
    return vals32 * inv_rms, inv_rms


def rms_back(normed, inv_rms, grad_out):
    return inv_rms * (grad_out - normed * jnp.mean(grad_out * normed, axis=-1, keepdims=True))


def gelu_tanh(values):
    return jax.nn.gelu(values, approximate=True)


def gelu_back(pre_act, grad_out):
    return jax.vjp(gelu_tanh, pre_act)[1](grad_out)[0]


def mat_mul(subscripts, lhs_arr, rhs_arr):
    return jnp.einsum(subscripts, lhs_arr, rhs_arr, preferred_element_type=jnp.float32)


def dot_f32(lhs, rhs):
    return jnp.dot(lhs, rhs, preferred_element_type=jnp.float32)


def dot_rows(lhs, rhs):
    return lax.dot_general(lhs, rhs, (((1,), (1,)), ((), ())), preferred_element_type=jnp.float32)


def valid_cols(core, blk, half_cols):
    cols = blk * BLK + lax.broadcasted_iota(jnp.int32, (1, BLK), 1)
    return (cols >= 64 * core) & (cols < half_cols + 64 * core)


def join_rows(pieces, dst):
    for j, piece in enumerate(pieces):
        dst[j * PIECE:(j + 1) * PIECE, :] = piece[...]


def piece_specs(first_blk, d_t, half_cols):
    def spec(j):
        def index(i, m):
            return jnp.clip(N_PIECE * (first_blk(m) + i) + j - m[0], 0, half_cols // PIECE - 1), 0

        return pl.BlockSpec((PIECE, d_t), index)

    return [spec(j) for j in range(N_PIECE)]


def stats_kernel(half_cols, meta, ht, rs, *refs):
    pieces, refs = refs[:N_PIECE], refs[N_PIECE:]
    ws, zt_out, zs_out, st_out, mt, st, at, ms, ss, wt = refs
    join_rows(pieces, wt)
    blk = pl.program_id(0)
    valid = valid_cols(meta[0], blk, half_cols)

    @pl.when(blk == 0)
    def _():
        mt[...] = jnp.full_like(mt, NEG)
        ms[...] = jnp.full_like(ms, NEG)
        st[...] = jnp.zeros_like(st)
        at[...] = jnp.zeros_like(at)
        ss[...] = jnp.zeros_like(ss)

    rows_all = ht.shape[0]
    step = 512
    for row in range(0, rows_all, step):
        rows = pl.ds(row, step)
        zt = jnp.where(valid, dot_rows(ht[rows, :], wt[...]), NEG)
        zs = jnp.where(valid, dot_f32(rs[rows, :], ws[...]), NEG)
        zt_out[rows, :] = zt
        zs_out[rows, :] = zs
        parts_t = [zt[:, j:j + 128] for j in range(0, BLK, 128)]
        parts_s = [zs[:, j:j + 128] for j in range(0, BLK, 128)]
        m_old = mt[rows, :]
        m_new = functools.reduce(jnp.maximum, parts_t, m_old)
        corr = jnp.exp(m_old - m_new)
        exps = [jnp.exp(p - m_new) for p in parts_t]
        st[rows, :] = st[rows, :] * corr + sum(exps)
        at[rows, :] = at[rows, :] * corr + sum(e * (p - q) for e, p, q in zip(exps, parts_t, parts_s))
        mt[rows, :] = m_new
        m_old = ms[rows, :]
        m_new = functools.reduce(jnp.maximum, parts_s, m_old)
        corr = jnp.exp(m_old - m_new)
        ss[rows, :] = ss[rows, :] * corr + sum(jnp.exp(p - m_new) for p in parts_s)
        ms[rows, :] = m_new

    @pl.when(blk == pl.num_programs(0) - 1)
    def _():
        top_t = jnp.max(mt[...], axis=-1, keepdims=True)
        scale = jnp.exp(mt[...] - top_t)
        sum_t = jnp.sum(st[...] * scale, axis=-1, keepdims=True)
        sum_a = jnp.sum(at[...] * scale, axis=-1, keepdims=True)
        top_s = jnp.max(ms[...], axis=-1, keepdims=True)
        sum_s = jnp.sum(ss[...] * jnp.exp(ms[...] - top_s), axis=-1, keepdims=True)
        lane = lax.broadcasted_iota(jnp.int32, st_out.shape, 1)
        res = jnp.where(lane == 0, top_t, jnp.where(lane == 1, sum_t, sum_a))
        res = jnp.where(lane == 3, top_s, jnp.where(lane == 4, sum_s, res))
        st_out[...] = res


def head_stats(meta, ht, rs, hts, head_s, half_cols):
    rows, d_t = ht.shape
    d_s = rs.shape[1]
    cols = N_BLK * BLK
    grid_spec = pltpu.PrefetchScalarGridSpec(
        num_scalar_prefetch=1,
        grid=(N_BLK,),
        in_specs=[
            pl.BlockSpec((rows, d_t), lambda k, m: (0, 0), pipeline_mode=pl.Buffered(1)),
            pl.BlockSpec((rows, d_s), lambda k, m: (0, 0), pipeline_mode=pl.Buffered(1)),
            *piece_specs(lambda m: 0, d_t, half_cols),
            pl.BlockSpec((d_s, BLK), lambda k, m: (0, k + (N_BLK - 1) * m[0])),
        ],
        out_specs=[
            pl.BlockSpec((rows, BLK), lambda k, m: (0, k)),
            pl.BlockSpec((rows, BLK), lambda k, m: (0, k)),
            pl.BlockSpec((rows, 128), lambda k, m: (0, 0)),
        ],
        scratch_shapes=[pltpu.VMEM((rows, 128), jnp.float32)] * 5 + [pltpu.VMEM((BLK, d_t), jnp.bfloat16)],
    )
    return pl.pallas_call(
        functools.partial(stats_kernel, half_cols),
        grid_spec=grid_spec,
        out_shape=[
            jax.ShapeDtypeStruct((rows, cols), jnp.float32),
            jax.ShapeDtypeStruct((rows, cols), jnp.float32),
            jax.ShapeDtypeStruct((rows, 128), jnp.float32),
        ],
        compiler_params=pltpu.CompilerParams(dimension_semantics=("arbitrary",), vmem_limit_bytes=VMEM_LIMIT),
        cost_estimate=pl.CostEstimate(
            flops=2 * rows * cols * (d_t + d_s), bytes_accessed=cols * (2 * (d_t + d_s) + 8 * rows),
            transcendentals=2 * rows * cols),
        name="head_stats",
    )(meta, ht, rs, *([hts] * N_PIECE), head_s)


def logit_grad(zt, zs, lse_t, lse_s, coef):
    return (coef * (jnp.exp(zs - lse_s) - jnp.exp(zt - lse_t))).astype(jnp.bfloat16)


def grad_kernel(half_cols, coef, meta, ht, rs, rst, lt, ls, *refs):
    ws, zt_own, zs_own, out, wt = refs[N_PIECE:]
    join_rows(refs[:N_PIECE], wt)
    own = meta[1]
    valid = valid_cols(meta[0], meta[2] + pl.program_id(0), half_cols)
    lg = logit_grad(zt_own[...], zs_own[...], lt[own], ls[own], coef)
    out[...] = dot_f32(rst[own], lg)
    for other in range(1, 4):
        grp = lax.rem(own + other, 4)
        zt = jnp.where(valid, dot_rows(ht[grp], wt[...]), NEG)
        zs = jnp.where(valid, dot_f32(rs[grp], ws[...]), NEG)
        out[...] += dot_f32(rst[grp], logit_grad(zt, zs, lt[grp], ls[grp], coef))


def head_grad_blocks(n_blocks, meta, ht_all, rs_all, rst_all, lse_t, lse_s, hts, head_s, zt, zs, half_cols, coef):
    groups, rows, d_t = ht_all.shape
    d_s = rs_all.shape[2]

    def whole(shape):
        return pl.BlockSpec(shape, lambda i, m: (0,) * len(shape), pipeline_mode=pl.Buffered(1))

    grid_spec = pltpu.PrefetchScalarGridSpec(
        num_scalar_prefetch=1,
        grid=(n_blocks,),
        in_specs=[
            whole((groups, rows, d_t)),
            whole((groups, rows, d_s)),
            whole((groups, d_s, rows)),
            whole((groups, rows, 1)),
            whole((groups, rows, 1)),
            *piece_specs(lambda m: m[2], d_t, half_cols),
            pl.BlockSpec((d_s, BLK), lambda i, m: (0, m[2] + i + (N_BLK - 1) * m[0])),
            pl.BlockSpec((rows, BLK), lambda i, m: (0, m[2] + i)),
            pl.BlockSpec((rows, BLK), lambda i, m: (0, m[2] + i)),
        ],
        out_specs=pl.BlockSpec((d_s, BLK), lambda i, m: (0, i)),
        scratch_shapes=[pltpu.VMEM((BLK, d_t), jnp.bfloat16)],
    )
    cols = n_blocks * BLK
    return pl.pallas_call(
        functools.partial(grad_kernel, half_cols, coef),
        grid_spec=grid_spec,
        out_shape=jax.ShapeDtypeStruct((d_s, cols), jnp.float32),
        compiler_params=pltpu.CompilerParams(dimension_semantics=("arbitrary",), vmem_limit_bytes=VMEM_LIMIT),
        cost_estimate=pl.CostEstimate(
            flops=2 * rows * cols * (3 * d_t + 7 * d_s), bytes_accessed=cols * (2 * d_t + 6 * d_s + 8 * rows),
            transcendentals=8 * rows * cols),
        name="head_grad",
    )(meta, ht_all, rs_all, rst_all, lse_t, lse_s, *([hts] * N_PIECE), head_s, zt, zs)


def input_grad_kernel(coef, meta, lt, ls, zt, zs, ws, out):
    blk = pl.program_id(0)
    last = pl.num_programs(0) - 1

    @pl.when(blk == 0)
    def _():
        out[...] = jnp.zeros_like(out)

    @pl.when(blk < last)
    def _():
        lg = logit_grad(zt[...], zs[...], lt[...], ls[...], coef)
        out[...] += dot_rows(lg, ws[...])

    @pl.when(blk == last)
    def _():
        lg = logit_grad(zt[:, :128], zs[:, :128], lt[...], ls[...], coef)
        out[...] += dot_rows(lg, ws[:, :128])


def head_input_grad(meta, lse_t, lse_s, zt, zs, head_s, coef):
    rows = zt.shape[0]
    d_s = head_s.shape[0]
    cols = N_BLK * BLK
    grid_spec = pltpu.PrefetchScalarGridSpec(
        num_scalar_prefetch=1,
        grid=(N_BLK,),
        in_specs=[
            pl.BlockSpec((rows, 1), lambda k, m: (0, 0)),
            pl.BlockSpec((rows, 1), lambda k, m: (0, 0)),
            pl.BlockSpec((rows, BLK), lambda k, m: (0, k)),
            pl.BlockSpec((rows, BLK), lambda k, m: (0, k)),
            pl.BlockSpec((d_s, BLK), lambda k, m: (0, k + (N_BLK - 1) * m[0])),
        ],
        out_specs=pl.BlockSpec((rows, d_s), lambda k, m: (0, 0)),
    )
    return pl.pallas_call(
        functools.partial(input_grad_kernel, coef),
        grid_spec=grid_spec,
        out_shape=jax.ShapeDtypeStruct((rows, d_s), jnp.float32),
        compiler_params=pltpu.CompilerParams(dimension_semantics=("arbitrary",), vmem_limit_bytes=VMEM_LIMIT),
        cost_estimate=pl.CostEstimate(
            flops=4 * rows * cols * d_s, bytes_accessed=cols * (2 * d_s + 8 * rows), transcendentals=2 * rows * cols),
        name="head_input_grad",
    )(meta, lse_t, lse_s, zt, zs, head_s)


def block_pieces():
    shared = []
    for part, n_blocks in enumerate(OWN_SPLIT):
        for j in range(n_blocks):
            shared.append((part, j))
    pieces = {}
    for k in range(N_SHARED):
        part, j = shared[k % N_OWN]
        pieces[k] = (part, k // N_OWN, j * BLK)
    k = N_SHARED
    for part, n_blocks in enumerate(RED_SPLIT):
        for j in range(n_blocks):
            pieces[k] = (len(OWN_SPLIT) + part, None, j * BLK)
            k += 1
    return pieces


def piece_view(refs, piece, extra, width):
    part, lead, col = piece
    ref = refs[part]
    if lead is None:
        return ref.at[:, pl.ds(col + extra, width)]
    return ref.at[lead, :, pl.ds(col + extra, width)]


def assemble_kernel(n_arr, n_buf, meta, *refs):
    own, partner = refs[:n_arr], refs[n_arr:2 * n_arr]
    out, bufs, seam_a, seam_b, in_sem, out_sem, seam_sem = refs[2 * n_arr:]
    core = meta[0]
    pieces = block_pieces()
    seam_col = (N_BLK - 1) * BLK
    jobs = [(0, pieces[k], 0, k * BLK, BLK) for k in range(N_BLK - 1)]
    jobs.append((1, pieces[0], 128, seam_col + 128, BLK - 128))
    jobs += [(1, pieces[k], 0, seam_col + k * BLK, BLK) for k in range(1, N_BLK - 1)]
    jobs.append((1, pieces[N_BLK - 1], 0, seam_col + (N_BLK - 1) * BLK, 128))

    def fetch(half, piece, extra, width, dst, sem):
        @pl.when(core == half)
        def _():
            pltpu.make_async_copy(piece_view(own, piece, extra, width), dst, sem).start()

        @pl.when(core != half)
        def _():
            pltpu.make_async_copy(piece_view(partner, piece, extra, width), dst, sem).start()

    fetch(0, pieces[N_BLK - 1], 0, 128, seam_a, seam_sem.at[0])
    fetch(1, pieces[0], 0, 128, seam_b, seam_sem.at[1])

    def buf_of(i):
        return bufs.at[i % n_buf, :, pl.ds(0, jobs[i][4])]

    def start_in(i):
        half, piece, extra, _, width = jobs[i]
        fetch(half, piece, extra, width, buf_of(i), in_sem.at[i % n_buf])

    def out_copy(i):
        return pltpu.make_async_copy(buf_of(i), out.at[:, pl.ds(jobs[i][3], jobs[i][4])], out_sem.at[i % n_buf])

    def finish_in(i):
        pltpu.make_async_copy(buf_of(i), buf_of(i), in_sem.at[i % n_buf]).wait()
        out_copy(i).start()

    lag = n_buf // 2
    for i in range(len(jobs) + lag):
        if i < len(jobs):
            if i >= n_buf:
                out_copy(i - n_buf).wait()
            start_in(i)
        if i >= lag:
            finish_in(i - lag)
    pltpu.make_async_copy(seam_a, seam_a, seam_sem.at[0]).wait()
    pltpu.make_async_copy(seam_b, seam_b, seam_sem.at[1]).wait()
    seam_a[...] += seam_b[...]
    seam = pltpu.make_async_copy(seam_a, out.at[:, pl.ds(seam_col, 128)], seam_sem.at[0])
    seam.start()
    for i in range(len(jobs) - n_buf, len(jobs)):
        out_copy(i).wait()
    seam.wait()


def assemble(meta, own, partner, vocab):
    d_s = own[0].shape[-2]
    n_buf = 8
    any_spec = pl.BlockSpec(memory_space=pl.ANY)
    return pl.pallas_call(
        functools.partial(assemble_kernel, len(own), n_buf),
        in_specs=[pl.BlockSpec(memory_space=pltpu.SMEM)] + [any_spec] * (2 * len(own)),
        out_specs=any_spec,
        out_shape=jax.ShapeDtypeStruct((d_s, vocab), jnp.float32),
        scratch_shapes=[
            pltpu.VMEM((n_buf, d_s, BLK), jnp.float32),
            pltpu.VMEM((d_s, 128), jnp.float32),
            pltpu.VMEM((d_s, 128), jnp.float32),
            pltpu.SemaphoreType.DMA((n_buf,)),
            pltpu.SemaphoreType.DMA((n_buf,)),
            pltpu.SemaphoreType.DMA((2,)),
        ],
        compiler_params=pltpu.CompilerParams(vmem_limit_bytes=VMEM_LIMIT),
        cost_estimate=pl.CostEstimate(flops=d_s * vocab * 100, bytes_accessed=8 * d_s * vocab, transcendentals=0),
        name="assemble",
    )(meta, *own, *partner)


def teacher_kernel(n_layers, x, gain, w_up, w_down, h_out, ht_out, up_buf, down_buf, n_own, n_oth, act_own, act_oth,
                   part_own, part_oth, part_in, w_sem, n_send, n_recv, p_send, p_recv):
    core = lax.axis_index('tp')
    other = {'tp': 1 - core}
    mesh_id = pl.DeviceIdType.MESH
    barrier = pltpu.get_barrier_semaphore()
    pl.semaphore_signal(barrier, inc=1, device_id=other, device_id_type=mesh_id)
    pl.semaphore_wait(barrier, 1)

    def fetch(layer, slot):
        return (pltpu.make_async_copy(w_up.at[layer], up_buf.at[slot], w_sem.at[0, slot]),
                pltpu.make_async_copy(w_down.at[layer], down_buf.at[slot], w_sem.at[1, slot]))

    def norm_exchange():
        return pltpu.make_async_remote_copy(src_ref=n_own, dst_ref=n_oth, send_sem=n_send, recv_sem=n_recv,
                                            device_id=other, device_id_type=mesh_id)

    for copy in fetch(0, 0):
        copy.start()
    h_out[...] = x[...]
    d_ff = up_buf.shape[2]
    rows_all = x.shape[0]
    half_rows = rows_all // 2

    def up_proj(src, dst, slot):
        for col in range(0, d_ff, 512):
            pre = dot_f32(src[...], up_buf[slot, :, col:col + 512])
            dst[:, col:col + 512] = gelu_tanh(pre).astype(jnp.bfloat16)

    def layer_step(layer, carry):
        slot = lax.rem(layer, 2)

        @pl.when(layer + 1 < n_layers)
        def _():
            for copy in fetch(layer + 1, 1 - slot):
                copy.start()

        n_own[...] = (rms_parts(h_out[...])[0] * gain[pl.ds(layer, 1), :]).astype(jnp.bfloat16)
        give = norm_exchange()
        give.start()
        up_copy, down_copy = fetch(layer, slot)
        up_copy.wait()
        up_proj(n_own, act_own, slot)
        give.wait_recv()
        up_proj(n_oth, act_oth, slot)
        down_copy.wait()
        sends = []
        for half in range(2):
            rows = pl.ds(half * half_rows, half_rows)
            part_oth[rows, :] = dot_f32(act_oth[rows, :], down_buf[slot])
            sends.append(pltpu.make_async_remote_copy(
                src_ref=part_oth.at[rows, :], dst_ref=part_in.at[rows, :], send_sem=p_send.at[half],
                recv_sem=p_recv.at[half], device_id=other, device_id_type=mesh_id))
            sends[-1].start()
        for half in range(2):
            rows = pl.ds(half * half_rows, half_rows)
            part_own[rows, :] = dot_f32(act_own[rows, :], down_buf[slot])
        for half in range(2):
            rows = pl.ds(half * half_rows, half_rows)
            sends[half].wait_recv()
            layer_out = (part_own[rows, :] + part_in[rows, :]).astype(jnp.bfloat16).astype(jnp.float32)
            h_out[rows, :] = (h_out[rows, :].astype(jnp.float32) + layer_out).astype(jnp.bfloat16)
        for half in range(2):
            sends[half].wait_send()
        give.wait_send()
        return carry

    lax.fori_loop(0, n_layers, layer_step, 0)
    n_own[...] = rms_parts(h_out[...])[0].astype(jnp.bfloat16)
    give = norm_exchange()
    give.start()
    ht_out[core] = n_own[...]
    give.wait_recv()
    ht_out[1 - core] = n_oth[...]
    give.wait_send()


def teacher(x, gain, w_up, w_down):
    rows, d_t = x.shape
    n_layers, _, d_ff = w_up.shape
    vmem = pl.BlockSpec(memory_space=pltpu.VMEM)
    any_spec = pl.BlockSpec(memory_space=pl.ANY)
    return pl.pallas_call(
        functools.partial(teacher_kernel, n_layers),
        in_specs=[vmem, vmem, any_spec, any_spec],
        out_specs=[vmem, vmem],
        out_shape=[jax.ShapeDtypeStruct((rows, d_t), jnp.bfloat16),
                   jax.ShapeDtypeStruct((2, rows, d_t), jnp.bfloat16)],
        scratch_shapes=[
            pltpu.VMEM((2, d_t, d_ff), jnp.bfloat16),
            pltpu.VMEM((2, d_ff, d_t), jnp.bfloat16),
            pltpu.VMEM((rows, d_t), jnp.bfloat16),
            pltpu.VMEM((rows, d_t), jnp.bfloat16),
            pltpu.VMEM((rows, d_ff), jnp.bfloat16),
            pltpu.VMEM((rows, d_ff), jnp.bfloat16),
            pltpu.VMEM((rows, d_t), jnp.float32),
            pltpu.VMEM((rows, d_t), jnp.float32),
            pltpu.VMEM((rows, d_t), jnp.float32),
            pltpu.SemaphoreType.DMA((2, 2)),
            pltpu.SemaphoreType.DMA,
            pltpu.SemaphoreType.DMA,
            pltpu.SemaphoreType.DMA((2,)),
            pltpu.SemaphoreType.DMA((2,)),
        ],
        compiler_params=pltpu.CompilerParams(collective_id=0, has_side_effects=True, vmem_limit_bytes=VMEM_LIMIT),
        cost_estimate=pl.CostEstimate(flops=8 * n_layers * rows * d_t * d_ff, bytes_accessed=4 * n_layers * d_t * d_ff,
                                      transcendentals=2 * n_layers * rows * d_ff),
        name="teacher",
    )(x, gain, w_up, w_down)


def after(value, *earlier):
    return lax.optimization_barrier((value, *earlier))[0]


def solution(mesh):
    dp_size = mesh.shape['dp']
    tp_size = mesh.shape['tp']
    swap = [(0, 1), (1, 0)]

    def local_step(x_teach, x_stud, w_up_t, w_down_t, gain_t, head_t, w_up_s, w_down_s, gain_s, proj_s, head_s):
        dp_idx = lax.axis_index('dp')
        core = lax.axis_index('tp')
        n_seq, seq_len, d_s = x_stud.shape
        d_t = x_teach.shape[-1]
        local_tok = n_seq * seq_len
        group_tok = local_tok * tp_size
        n_tokens = group_tok * dp_size
        half_cols = head_t.shape[1]
        vocab = head_s.shape[1]
        feat_coef = 1.0 / (n_tokens * d_t)
        kl_coef = 1.0 / n_tokens
        w_up, w_down, gain, proj = w_up_s[0], w_down_s[0], gain_s[0], proj_s[0]
        both = ('dp', 'tp')

        x_all = lax.all_gather(x_stud.reshape(local_tok, d_s), both, axis=0, tiled=True)
        norm_all, _ = rms_parts(x_all)
        n_all = (norm_all * gain).astype(jnp.bfloat16)

        norm_cur, _ = rms_parts(x_stud.reshape(local_tok, d_s))
        normed = (norm_cur * gain).astype(jnp.bfloat16)
        hidden_s = gelu_tanh(mat_mul('sd,df->sf', normed, w_up)).astype(jnp.bfloat16)
        residual = x_stud.reshape(local_tok, d_s).astype(jnp.float32) + mat_mul('sf,fd->sd', hidden_s, w_down)
        norm_next, inv_next = rms_parts(residual)
        proj_in = norm_next.astype(jnp.bfloat16)
        proj_out = mat_mul('sd,de->se', proj_in, proj)
        rs_flat = lax.all_gather(proj_in, both, axis=0, tiled=True)
        rs_all = rs_flat.reshape(dp_size, group_tok, d_s)
        rst_all = jnp.swapaxes(rs_all, 1, 2)
        rs_grp = lax.dynamic_index_in_dim(rs_all, dp_idx, 0, keepdims=False)

        hts = head_t.T

        f_half = w_up.shape[1] // tp_size
        up_half = lax.dynamic_slice_in_dim(w_up, core * f_half, f_half, axis=1)
        down_half = lax.dynamic_slice_in_dim(w_down, core * f_half, f_half, axis=0)
        pre_half = mat_mul('sd,df->sf', n_all, up_half)
        act_half = gelu_tanh(pre_half).astype(jnp.bfloat16)

        n_seq_t, half_seq, _ = x_teach.shape
        hidden, ht_pair = teacher(x_teach.reshape(-1, d_t), gain_t, w_up_t, w_down_t)
        feature = lax.all_to_all(hidden.reshape(n_seq_t, half_seq, d_t), 'tp', 0, 1, tiled=True)
        ht_grp = jnp.swapaxes(ht_pair.reshape(tp_size, n_seq_t, half_seq, d_t), 0, 1).reshape(group_tok, d_t)
        ht_all = lax.all_gather(ht_grp, 'dp')

        meta0 = jnp.stack([core, dp_idx, jnp.int32(0)]).astype(jnp.int32)
        zt, zs, stats = head_stats(meta0, ht_grp, rs_grp, hts, head_s, half_cols)
        stats_all = lax.all_gather(stats[:, :8].T, both).reshape(dp_size, tp_size, 8, group_tok)
        top_t, sum_t, sum_a, top_s, sum_s = [stats_all[:, :, j, :] for j in range(5)]
        max_t = jnp.max(top_t, axis=1)
        max_s = jnp.max(top_s, axis=1)
        scale_t = jnp.exp(top_t - max_t[:, None])
        all_t = jnp.sum(sum_t * scale_t, axis=1)
        all_a = jnp.sum(sum_a * scale_t, axis=1)
        all_s = jnp.sum(sum_s * jnp.exp(top_s - max_s[:, None]), axis=1)
        lse_t = max_t + jnp.log(all_t)
        lse_s = max_s + jnp.log(all_s)
        kl_total = jnp.sum(all_a / all_t - lse_t + lse_s)
        lse_t = lse_t[..., None]
        lse_s = lse_s[..., None]

        def blocks(base, count, lse):
            meta = jnp.stack([core, dp_idx, base]).astype(jnp.int32)
            return head_grad_blocks(count, meta, ht_all, rs_all, rst_all, lse, lse_s, hts, head_s, zt, zs,
                                    half_cols, kl_coef)

        own_parts = []
        base, lse_o = dp_idx * N_OWN, lse_t
        for count in OWN_SPLIT:
            own_parts.append(blocks(base, count, lse_o))
            base = base + count
            lse_o = after(lse_t, own_parts[-1])
        shared = []
        for part in own_parts:
            shared.append(lax.all_gather(part, 'dp'))

        lse_own_t = lax.dynamic_index_in_dim(lse_o, dp_idx, 0, keepdims=False)
        lse_own_s = lax.dynamic_index_in_dim(lse_s, dp_idx, 0, keepdims=False)
        full_in_grad = head_input_grad(meta0, lse_own_t, lse_own_s, zt, zs, head_s, kl_coef)
        give = lax.dynamic_slice_in_dim(full_in_grad, (1 - core) * local_tok, local_tok, axis=0)
        keep = lax.dynamic_slice_in_dim(full_in_grad, core * local_tok, local_tok, axis=0)
        head_in_grad = keep + lax.ppermute(give, 'tp', swap)

        feat_err = proj_out - feature.reshape(local_tok, d_t)
        err_total = jnp.sum(feat_err * feat_err)
        err_grad = (2.0 * feat_coef * feat_err).astype(jnp.bfloat16)
        out_grad = mat_mul('se,de->sd', err_grad, proj)
        resid_grad = rms_back(norm_next, inv_next, out_grad + head_in_grad)
        resid_all = lax.all_gather(resid_grad.astype(jnp.bfloat16), both, axis=0, tiled=True)
        err_all = lax.all_gather(err_grad, both, axis=0, tiled=True)

        lse_r = after(lse_t, full_in_grad)
        redundant = []
        base = jnp.int32(N_SHARED)
        for count in RED_SPLIT:
            redundant.append(blocks(base, count, lse_r))
            base = base + count
            lse_r = after(lse_t, redundant[-1])
        own = shared + redundant
        partner = []
        for part in own:
            partner.append(lax.ppermute(part, 'tp', swap))

        resid_all = after(resid_all, redundant[-1])
        act_grad = mat_mul('sd,fd->sf', resid_all, down_half)
        pre_grad = gelu_back(pre_half, act_grad).astype(jnp.bfloat16)
        up_part = mat_mul('sd,sf->df', n_all, pre_grad)
        down_part = mat_mul('sf,sd->fd', act_half, resid_all)
        e_half = d_t // tp_size
        proj_part = mat_mul('sd,se->de', rs_flat, lax.dynamic_slice_in_dim(err_all, core * e_half, e_half, axis=1))
        pre_own = lax.dynamic_slice_in_dim(pre_grad, dp_idx * group_tok, group_tok, axis=0)
        norm_own = lax.dynamic_slice_in_dim(norm_all, dp_idx * group_tok, group_tok, axis=0)
        gain_part = jnp.sum(mat_mul('sf,df->sd', pre_own, up_half) * norm_own, axis=0)

        grad_up = lax.all_gather(up_part, 'tp', axis=1, tiled=True)[None]
        grad_down = lax.all_gather(down_part, 'tp', axis=0, tiled=True)[None]
        grad_proj = lax.all_gather(proj_part, 'tp', axis=1, tiled=True)[None]
        small = jnp.concatenate([gain_part, err_total[None], jnp.zeros((1023 - d_s,), jnp.float32)]).reshape(8, 128)
        small = jnp.sum(lax.all_gather(small, both), axis=0).reshape(1024)
        grad_gain, err_sum = small[:d_s], small[d_s]
        loss = feat_coef * err_sum + kl_coef * kl_total
        head_grad = assemble(meta0, own, partner, vocab)
        return loss, grad_up, grad_down, grad_gain[None], grad_proj, head_grad

    in_specs = (P('dp', 'tp', None), P(('dp', 'tp'), None, None), P(None, None, 'tp'), P(None, 'tp', None),
                P(), P(None, 'tp'), P(), P(), P(), P(), P())
    out_specs = (P(), P(), P(), P(), P(), P())

    return jax.shard_map(local_step, mesh=mesh, in_specs=in_specs, out_specs=out_specs, check_vma=False)
```

```python
import functools

import jax
import jax.numpy as jnp
from jax import lax
from jax.experimental import pallas as pl
from jax.experimental.pallas import tpu as pltpu
from jax.sharding import PartitionSpec as P


NORM_EPS = 1e-6
NEG = -3.0e38
BLK = 512
PIECE = 64
N_PIECE = BLK // PIECE
N_BLK = 50
N_OWN = 7
N_SHARED = 4 * N_OWN
OWN_SPLIT = (4, 3)
RED_SPLIT = (7, 7, 8)
VMEM_LIMIT = 60 * 1024 * 1024


def rms_parts(values):
    vals32 = values.astype(jnp.float32)
    inv_rms = lax.rsqrt(jnp.mean(vals32 * vals32, axis=-1, keepdims=True) + NORM_EPS)
    return vals32 * inv_rms, inv_rms


def rms_back(normed, inv_rms, grad_out):
    return inv_rms * (grad_out - normed * jnp.mean(grad_out * normed, axis=-1, keepdims=True))


def gelu_tanh(values):
    return jax.nn.gelu(values, approximate=True)


def gelu_back(pre_act, grad_out):
    return jax.vjp(gelu_tanh, pre_act)[1](grad_out)[0]


def mat_mul(subscripts, lhs_arr, rhs_arr):
    return jnp.einsum(subscripts, lhs_arr, rhs_arr, preferred_element_type=jnp.float32)


def dot_f32(lhs, rhs):
    return jnp.dot(lhs, rhs, preferred_element_type=jnp.float32)


def dot_rows(lhs, rhs):
    return lax.dot_general(lhs, rhs, (((1,), (1,)), ((), ())), preferred_element_type=jnp.float32)


def valid_cols(core, blk, half_cols):
    cols = blk * BLK + lax.broadcasted_iota(jnp.int32, (1, BLK), 1)
    return (cols >= 64 * core) & (cols < half_cols + 64 * core)


def join_rows(pieces, dst):
    for j, piece in enumerate(pieces):
        dst[j * PIECE:(j + 1) * PIECE, :] = piece[...]


def piece_specs(first_blk, d_t, half_cols):
    def spec(j):
        def index(i, m):
            return jnp.clip(N_PIECE * (first_blk(m) + i) + j - m[0], 0, half_cols // PIECE - 1), 0

        return pl.BlockSpec((PIECE, d_t), index)

    return [spec(j) for j in range(N_PIECE)]


def stats_kernel(half_cols, meta, ht, rs, *refs):
    pieces, refs = refs[:N_PIECE], refs[N_PIECE:]
    ws, zt_out, zs_out, st_out, mt, st, at, ms, ss, wt = refs
    join_rows(pieces, wt)
    blk = pl.program_id(0)
    valid = valid_cols(meta[0], blk, half_cols)

    @pl.when(blk == 0)
    def _():
        mt[...] = jnp.full_like(mt, NEG)
        ms[...] = jnp.full_like(ms, NEG)
        st[...] = jnp.zeros_like(st)
        at[...] = jnp.zeros_like(at)
        ss[...] = jnp.zeros_like(ss)

    rows_all = ht.shape[0]
    step = 512
    for row in range(0, rows_all, step):
        rows = pl.ds(row, step)
        zt = jnp.where(valid, dot_rows(ht[rows, :], wt[...]), NEG)
        zs = jnp.where(valid, dot_f32(rs[rows, :], ws[...]), NEG)
        zt_out[rows, :] = zt
        zs_out[rows, :] = zs
        parts_t = [zt[:, j:j + 128] for j in range(0, BLK, 128)]
        parts_s = [zs[:, j:j + 128] for j in range(0, BLK, 128)]
        m_old = mt[rows, :]
        m_new = functools.reduce(jnp.maximum, parts_t, m_old)
        corr = jnp.exp(m_old - m_new)
        exps = [jnp.exp(p - m_new) for p in parts_t]
        st[rows, :] = st[rows, :] * corr + sum(exps)
        at[rows, :] = at[rows, :] * corr + sum(e * (p - q) for e, p, q in zip(exps, parts_t, parts_s))
        mt[rows, :] = m_new
        m_old = ms[rows, :]
        m_new = functools.reduce(jnp.maximum, parts_s, m_old)
        corr = jnp.exp(m_old - m_new)
        ss[rows, :] = ss[rows, :] * corr + sum(jnp.exp(p - m_new) for p in parts_s)
        ms[rows, :] = m_new

    @pl.when(blk == pl.num_programs(0) - 1)
    def _():
        top_t = jnp.max(mt[...], axis=-1, keepdims=True)
        scale = jnp.exp(mt[...] - top_t)
        sum_t = jnp.sum(st[...] * scale, axis=-1, keepdims=True)
        sum_a = jnp.sum(at[...] * scale, axis=-1, keepdims=True)
        top_s = jnp.max(ms[...], axis=-1, keepdims=True)
        sum_s = jnp.sum(ss[...] * jnp.exp(ms[...] - top_s), axis=-1, keepdims=True)
        lane = lax.broadcasted_iota(jnp.int32, st_out.shape, 1)
        res = jnp.where(lane == 0, top_t, jnp.where(lane == 1, sum_t, sum_a))
        res = jnp.where(lane == 3, top_s, jnp.where(lane == 4, sum_s, res))
        st_out[...] = res


def head_stats(meta, ht, rs, hts, head_s, half_cols):
    rows, d_t = ht.shape
    d_s = rs.shape[1]
    cols = N_BLK * BLK
    grid_spec = pltpu.PrefetchScalarGridSpec(
        num_scalar_prefetch=1,
        grid=(N_BLK,),
        in_specs=[
            pl.BlockSpec((rows, d_t), lambda k, m: (0, 0), pipeline_mode=pl.Buffered(1)),
            pl.BlockSpec((rows, d_s), lambda k, m: (0, 0), pipeline_mode=pl.Buffered(1)),
            *piece_specs(lambda m: 0, d_t, half_cols),
            pl.BlockSpec((d_s, BLK), lambda k, m: (0, k + (N_BLK - 1) * m[0])),
        ],
        out_specs=[
            pl.BlockSpec((rows, BLK), lambda k, m: (0, k)),
            pl.BlockSpec((rows, BLK), lambda k, m: (0, k)),
            pl.BlockSpec((rows, 128), lambda k, m: (0, 0)),
        ],
        scratch_shapes=[pltpu.VMEM((rows, 128), jnp.float32)] * 5 + [pltpu.VMEM((BLK, d_t), jnp.bfloat16)],
    )
    return pl.pallas_call(
        functools.partial(stats_kernel, half_cols),
        grid_spec=grid_spec,
        out_shape=[
            jax.ShapeDtypeStruct((rows, cols), jnp.float32),
            jax.ShapeDtypeStruct((rows, cols), jnp.float32),
            jax.ShapeDtypeStruct((rows, 128), jnp.float32),
        ],
        compiler_params=pltpu.CompilerParams(dimension_semantics=("arbitrary",), vmem_limit_bytes=VMEM_LIMIT),
        cost_estimate=pl.CostEstimate(
            flops=2 * rows * cols * (d_t + d_s), bytes_accessed=cols * (2 * (d_t + d_s) + 8 * rows),
            transcendentals=2 * rows * cols),
        name="head_stats",
    )(meta, ht, rs, *([hts] * N_PIECE), head_s)


def logit_grad(zt, zs, lse_t, lse_s, coef):
    return (coef * (jnp.exp(zs - lse_s) - jnp.exp(zt - lse_t))).astype(jnp.bfloat16)


def grad_kernel(half_cols, coef, hook, meta, ht, rs, rst, lt, ls, *refs):
    ws, zt_own, zs_own = refs[N_PIECE:N_PIECE + 3]
    extra, refs = refs[N_PIECE + 3:len(refs) - hook.n_tail], refs[:N_PIECE] + refs[len(refs) - hook.n_tail:]
    out, wt = hook.bind(meta, extra, refs[N_PIECE:])
    hook(0)
    join_rows(refs[:N_PIECE], wt)
    own = meta[1]
    valid = valid_cols(meta[0], meta[2] + pl.program_id(0), half_cols)
    lg = logit_grad(zt_own[...], zs_own[...], lt[own], ls[own], coef)
    out[...] = dot_f32(rst[own], lg)
    hook(1)
    for other in range(1, 4):
        grp = lax.rem(own + other, 4)
        zt = jnp.where(valid, dot_rows(ht[grp], wt[...]), NEG)
        zs = jnp.where(valid, dot_f32(rs[grp], ws[...]), NEG)
        out[...] += dot_f32(rst[grp], logit_grad(zt, zs, lt[grp], ls[grp], coef))
        hook(1 + other)


class NoCopies:
    n_tail = 2

    def bind(self, meta, extra, tail):
        return tail

    def __call__(self, point):
        pass


class BlockCopies:
    n_tail = 6

    def __init__(self, n_arr, jobs, n_steps, batch):
        self.n_arr, self.jobs, self.n_steps, self.batch = n_arr, jobs, n_steps, batch

    def bind(self, meta, extra, tail):
        self.core = meta[0]
        self.own, self.partner = extra[:self.n_arr], extra[self.n_arr:]
        out, self.full, wt, self.bufs, self.in_sem, self.out_sem = tail
        return out, wt

    def start_in(self, slot, job):
        kind, half, k = job
        piece, dst, sem = block_pieces()[k], self.bufs.at[slot], self.in_sem.at[slot]
        if kind == 'own':
            pltpu.make_async_copy(piece_view(self.own, piece, 0, BLK), dst, sem).start()
            return

        @pl.when(self.core == half)
        def _():
            pltpu.make_async_copy(piece_view(self.own, piece, 0, BLK), dst, sem).start()

        @pl.when(self.core != half)
        def _():
            pltpu.make_async_copy(piece_view(self.partner, piece, 0, BLK), dst, sem).start()

    def out_copy(self, slot, job):
        _, half, k = job
        half = self.core if half is None else half
        col = pl.multiple_of((N_BLK - 1) * BLK * half + k * BLK, 128)
        return pltpu.make_async_copy(self.bufs.at[slot], self.full.at[:, pl.ds(col, BLK)], self.out_sem.at[slot])

    def __call__(self, point):
        for step in range(self.n_steps):
            first = 2 * step * self.batch
            batches = (self.jobs[first:first + self.batch], self.jobs[first + self.batch:first + 2 * self.batch])

            @pl.when(pl.program_id(0) == step)
            def _(batches=batches):
                if point in (2, 4):
                    for slot, job in enumerate(batches[point // 2 - 1]):
                        self.out_copy(slot, job).wait()
                if point in (0, 2):
                    for slot, job in enumerate(batches[point // 2]):
                        self.start_in(slot, job)
                if point in (1, 3):
                    for slot, job in enumerate(batches[point // 2]):
                        pltpu.make_async_copy(self.bufs.at[slot], self.bufs.at[slot], self.in_sem.at[slot]).wait()
                        self.out_copy(slot, job).start()


EARLY_PARTS = (0, len(OWN_SPLIT))
EARLY_OWN_PART = len(OWN_SPLIT) + 1


def early_jobs():
    pieces = block_pieces()
    both = [('pair', half, k) for k in range(N_BLK) for half in range(2)
            if pieces[k][0] in EARLY_PARTS and (half, k) != (1, 0)]
    return both + [('own', None, k) for k in range(N_BLK) if pieces[k][0] == EARLY_OWN_PART]


def head_grad_blocks(n_blocks, meta, ht_all, rs_all, rst_all, lse_t, lse_s, hts, head_s, zt, zs, half_cols, coef,
                     own=None, partner=None):
    hook, extra = NoCopies(), ()
    out_specs = [pl.BlockSpec((head_s.shape[0], BLK), lambda i, m: (0, i))]
    out_shape = [jax.ShapeDtypeStruct((head_s.shape[0], n_blocks * BLK), jnp.float32)]
    scratch = [pltpu.VMEM((BLK, ht_all.shape[2]), jnp.bfloat16)]
    if own is not None:
        batch = 4
        extra = (*own, *partner)
        hook = BlockCopies(len(own), early_jobs(), n_blocks, batch)
        out_specs.append(pl.BlockSpec(memory_space=pl.ANY))
        out_shape.append(jax.ShapeDtypeStruct(head_s.shape, jnp.float32))
        scratch += [pltpu.VMEM((batch, head_s.shape[0], BLK), jnp.float32),
                    pltpu.SemaphoreType.DMA((batch,)), pltpu.SemaphoreType.DMA((batch,))]
    groups, rows, d_t = ht_all.shape
    d_s = rs_all.shape[2]

    def whole(shape):
        return pl.BlockSpec(shape, lambda i, m: (0,) * len(shape), pipeline_mode=pl.Buffered(1))

    grid_spec = pltpu.PrefetchScalarGridSpec(
        num_scalar_prefetch=1,
        grid=(n_blocks,),
        in_specs=[
            whole((groups, rows, d_t)),
            whole((groups, rows, d_s)),
            whole((groups, d_s, rows)),
            whole((groups, rows, 1)),
            whole((groups, rows, 1)),
            *piece_specs(lambda m: m[2], d_t, half_cols),
            pl.BlockSpec((d_s, BLK), lambda i, m: (0, m[2] + i + (N_BLK - 1) * m[0])),
            pl.BlockSpec((rows, BLK), lambda i, m: (0, m[2] + i)),
            pl.BlockSpec((rows, BLK), lambda i, m: (0, m[2] + i)),
        ] + [pl.BlockSpec(memory_space=pl.ANY)] * len(extra),
        out_specs=out_specs,
        scratch_shapes=scratch,
    )
    cols = n_blocks * BLK
    return pl.pallas_call(
        functools.partial(grad_kernel, half_cols, coef, hook),
        grid_spec=grid_spec,
        out_shape=out_shape,
        compiler_params=pltpu.CompilerParams(dimension_semantics=("arbitrary",), vmem_limit_bytes=VMEM_LIMIT),
        cost_estimate=pl.CostEstimate(
            flops=2 * rows * cols * (3 * d_t + 7 * d_s), bytes_accessed=cols * (2 * d_t + 6 * d_s + 8 * rows),
            transcendentals=8 * rows * cols),
        name="head_grad",
    )(meta, ht_all, rs_all, rst_all, lse_t, lse_s, *([hts] * N_PIECE), head_s, zt, zs, *extra)


def input_grad_kernel(coef, meta, lt, ls, zt, zs, ws, out):
    blk = pl.program_id(0)
    last = pl.num_programs(0) - 1

    @pl.when(blk == 0)
    def _():
        out[...] = jnp.zeros_like(out)

    @pl.when(blk < last)
    def _():
        step = 256
        for row in range(0, out.shape[0], step):
            rows = pl.ds(row, step)
            lg = logit_grad(zt[rows, :], zs[rows, :], lt[rows, :], ls[rows, :], coef)
            out[rows, :] += dot_rows(lg, ws[...])

    @pl.when(blk == last)
    def _():
        lg = logit_grad(zt[:, :128], zs[:, :128], lt[...], ls[...], coef)
        out[...] += dot_rows(lg, ws[:, :128])


def head_input_grad(meta, lse_t, lse_s, zt, zs, head_s, coef):
    rows = zt.shape[0]
    d_s = head_s.shape[0]
    cols = N_BLK * BLK
    grid_spec = pltpu.PrefetchScalarGridSpec(
        num_scalar_prefetch=1,
        grid=(N_BLK,),
        in_specs=[
            pl.BlockSpec((rows, 1), lambda k, m: (0, 0)),
            pl.BlockSpec((rows, 1), lambda k, m: (0, 0)),
            pl.BlockSpec((rows, BLK), lambda k, m: (0, k)),
            pl.BlockSpec((rows, BLK), lambda k, m: (0, k)),
            pl.BlockSpec((d_s, BLK), lambda k, m: (0, k + (N_BLK - 1) * m[0])),
        ],
        out_specs=pl.BlockSpec((rows, d_s), lambda k, m: (0, 0)),
    )
    return pl.pallas_call(
        functools.partial(input_grad_kernel, coef),
        grid_spec=grid_spec,
        out_shape=jax.ShapeDtypeStruct((rows, d_s), jnp.float32),
        compiler_params=pltpu.CompilerParams(dimension_semantics=("arbitrary",), vmem_limit_bytes=VMEM_LIMIT),
        cost_estimate=pl.CostEstimate(
            flops=4 * rows * cols * d_s, bytes_accessed=cols * (2 * d_s + 8 * rows), transcendentals=2 * rows * cols),
        name="head_input_grad",
    )(meta, lse_t, lse_s, zt, zs, head_s)


def block_pieces():
    shared = []
    for part, n_blocks in enumerate(OWN_SPLIT):
        for j in range(n_blocks):
            shared.append((part, j))
    pieces = {}
    for k in range(N_SHARED):
        part, j = shared[k % N_OWN]
        pieces[k] = (part, k // N_OWN, j * BLK)
    k = N_SHARED
    for part, n_blocks in enumerate(RED_SPLIT):
        for j in range(n_blocks):
            pieces[k] = (len(OWN_SPLIT) + part, None, j * BLK)
            k += 1
    return pieces


def piece_view(refs, piece, extra, width):
    part, lead, col = piece
    ref = refs[part]
    if lead is None:
        return ref.at[:, pl.ds(col + extra, width)]
    return ref.at[lead, :, pl.ds(col + extra, width)]


def assemble_kernel(n_arr, n_buf, meta, *refs):
    own, partner = refs[:n_arr], refs[n_arr:2 * n_arr]
    out, bufs, seam_a, seam_b, in_sem, out_sem, seam_sem = refs[2 * n_arr + 1:]
    core = meta[0]
    pieces = block_pieces()
    seam_col = (N_BLK - 1) * BLK
    late = [k for k in range(1, N_BLK - 1) if pieces[k][0] not in EARLY_PARTS + (EARLY_OWN_PART,)]
    jobs = [(half, pieces[k], 0, seam_col * half + k * BLK, BLK) for k in late for half in range(2)]
    jobs += [(None, pieces[k], 0, pl.multiple_of(seam_col * (1 - core) + k * BLK, 128), BLK)
             for k in range(N_BLK) if pieces[k][0] == EARLY_OWN_PART]
    jobs.append((1, pieces[0], 128, seam_col + 128, BLK - 128))
    jobs.append((1, pieces[N_BLK - 1], 0, seam_col + (N_BLK - 1) * BLK, 128))

    def fetch(half, piece, extra, width, dst, sem):
        if half is None:
            pltpu.make_async_copy(piece_view(partner, piece, extra, width), dst, sem).start()
            return

        @pl.when(core == half)
        def _():
            pltpu.make_async_copy(piece_view(own, piece, extra, width), dst, sem).start()

        @pl.when(core != half)
        def _():
            pltpu.make_async_copy(piece_view(partner, piece, extra, width), dst, sem).start()

    fetch(0, pieces[N_BLK - 1], 0, 128, seam_a, seam_sem.at[0])
    fetch(1, pieces[0], 0, 128, seam_b, seam_sem.at[1])

    def buf_of(i):
        return bufs.at[i % n_buf, :, pl.ds(0, jobs[i][4])]

    def start_in(i):
        half, piece, extra, _, width = jobs[i]
        fetch(half, piece, extra, width, buf_of(i), in_sem.at[i % n_buf])

    def out_copy(i):
        return pltpu.make_async_copy(buf_of(i), out.at[:, pl.ds(jobs[i][3], jobs[i][4])], out_sem.at[i % n_buf])

    def finish_in(i):
        pltpu.make_async_copy(buf_of(i), buf_of(i), in_sem.at[i % n_buf]).wait()
        out_copy(i).start()

    lag = n_buf // 2
    for i in range(len(jobs) + lag):
        if i < len(jobs):
            if i >= n_buf:
                out_copy(i - n_buf).wait()
            start_in(i)
        if i >= lag:
            finish_in(i - lag)
    pltpu.make_async_copy(seam_a, seam_a, seam_sem.at[0]).wait()
    pltpu.make_async_copy(seam_b, seam_b, seam_sem.at[1]).wait()
    seam_a[...] += seam_b[...]
    seam = pltpu.make_async_copy(seam_a, out.at[:, pl.ds(seam_col, 128)], seam_sem.at[0])
    seam.start()
    for i in range(len(jobs) - n_buf, len(jobs)):
        out_copy(i).wait()
    seam.wait()


def assemble(meta, own, partner, full, vocab):
    d_s = own[0].shape[-2]
    n_buf = 8
    any_spec = pl.BlockSpec(memory_space=pl.ANY)
    return pl.pallas_call(
        functools.partial(assemble_kernel, len(own), n_buf),
        in_specs=[pl.BlockSpec(memory_space=pltpu.SMEM)] + [any_spec] * (2 * len(own) + 1),
        out_specs=any_spec,
        out_shape=jax.ShapeDtypeStruct((d_s, vocab), jnp.float32),
        scratch_shapes=[
            pltpu.VMEM((n_buf, d_s, BLK), jnp.float32),
            pltpu.VMEM((d_s, 128), jnp.float32),
            pltpu.VMEM((d_s, 128), jnp.float32),
            pltpu.SemaphoreType.DMA((n_buf,)),
            pltpu.SemaphoreType.DMA((n_buf,)),
            pltpu.SemaphoreType.DMA((2,)),
        ],
        input_output_aliases={2 * len(own) + 1: 0},
        compiler_params=pltpu.CompilerParams(vmem_limit_bytes=VMEM_LIMIT),
        cost_estimate=pl.CostEstimate(flops=d_s * vocab * 100, bytes_accessed=8 * d_s * vocab, transcendentals=0),
        name="assemble",
    )(meta, *own, *partner, full)


def teacher_kernel(n_layers, x, gain, w_up, w_down, h_out, ht_out, up_buf, down_buf, n_own, n_oth, act_own, act_oth,
                   part_own, part_oth, part_in, w_sem, n_send, n_recv, p_send, p_recv):
    core = lax.axis_index('tp')
    other = {'tp': 1 - core}
    mesh_id = pl.DeviceIdType.MESH
    barrier = pltpu.get_barrier_semaphore()
    pl.semaphore_signal(barrier, inc=1, device_id=other, device_id_type=mesh_id)
    pl.semaphore_wait(barrier, 1)

    def fetch(layer, slot):
        return (pltpu.make_async_copy(w_up.at[layer], up_buf.at[slot], w_sem.at[0, slot]),
                pltpu.make_async_copy(w_down.at[layer], down_buf.at[slot], w_sem.at[1, slot]))

    def norm_exchange():
        return pltpu.make_async_remote_copy(src_ref=n_own, dst_ref=n_oth, send_sem=n_send, recv_sem=n_recv,
                                            device_id=other, device_id_type=mesh_id)

    for copy in fetch(0, 0):
        copy.start()
    h_out[...] = x[...]
    d_ff = up_buf.shape[2]
    rows_all = x.shape[0]
    half_rows = rows_all // 2

    def up_proj(src, dst, slot):
        for col in range(0, d_ff, 512):
            pre = dot_f32(src[...], up_buf[slot, :, col:col + 512])
            dst[:, col:col + 512] = gelu_tanh(pre).astype(jnp.bfloat16)

    def layer_step(layer, carry):
        slot = lax.rem(layer, 2)

        @pl.when(layer + 1 < n_layers)
        def _():
            for copy in fetch(layer + 1, 1 - slot):
                copy.start()

        n_own[...] = (rms_parts(h_out[...])[0] * gain[pl.ds(layer, 1), :]).astype(jnp.bfloat16)
        give = norm_exchange()
        give.start()
        up_copy, down_copy = fetch(layer, slot)
        up_copy.wait()
        up_proj(n_own, act_own, slot)
        give.wait_recv()
        up_proj(n_oth, act_oth, slot)
        down_copy.wait()
        sends = []
        for half in range(2):
            rows = pl.ds(half * half_rows, half_rows)
            part_oth[rows, :] = dot_f32(act_oth[rows, :], down_buf[slot])
            sends.append(pltpu.make_async_remote_copy(
                src_ref=part_oth.at[rows, :], dst_ref=part_in.at[rows, :], send_sem=p_send.at[half],
                recv_sem=p_recv.at[half], device_id=other, device_id_type=mesh_id))
            sends[-1].start()
        for half in range(2):
            rows = pl.ds(half * half_rows, half_rows)
            part_own[rows, :] = dot_f32(act_own[rows, :], down_buf[slot])
        for half in range(2):
            rows = pl.ds(half * half_rows, half_rows)
            sends[half].wait_recv()
            layer_out = (part_own[rows, :] + part_in[rows, :]).astype(jnp.bfloat16).astype(jnp.float32)
            h_out[rows, :] = (h_out[rows, :].astype(jnp.float32) + layer_out).astype(jnp.bfloat16)
        for half in range(2):
            sends[half].wait_send()
        give.wait_send()
        return carry

    lax.fori_loop(0, n_layers, layer_step, 0)
    n_own[...] = rms_parts(h_out[...])[0].astype(jnp.bfloat16)
    give = norm_exchange()
    give.start()
    ht_out[core] = n_own[...]
    give.wait_recv()
    ht_out[1 - core] = n_oth[...]
    give.wait_send()


def teacher(x, gain, w_up, w_down):
    rows, d_t = x.shape
    n_layers, _, d_ff = w_up.shape
    vmem = pl.BlockSpec(memory_space=pltpu.VMEM)
    any_spec = pl.BlockSpec(memory_space=pl.ANY)
    return pl.pallas_call(
        functools.partial(teacher_kernel, n_layers),
        in_specs=[vmem, vmem, any_spec, any_spec],
        out_specs=[vmem, vmem],
        out_shape=[jax.ShapeDtypeStruct((rows, d_t), jnp.bfloat16),
                   jax.ShapeDtypeStruct((2, rows, d_t), jnp.bfloat16)],
        scratch_shapes=[
            pltpu.VMEM((2, d_t, d_ff), jnp.bfloat16),
            pltpu.VMEM((2, d_ff, d_t), jnp.bfloat16),
            pltpu.VMEM((rows, d_t), jnp.bfloat16),
            pltpu.VMEM((rows, d_t), jnp.bfloat16),
            pltpu.VMEM((rows, d_ff), jnp.bfloat16),
            pltpu.VMEM((rows, d_ff), jnp.bfloat16),
            pltpu.VMEM((rows, d_t), jnp.float32),
            pltpu.VMEM((rows, d_t), jnp.float32),
            pltpu.VMEM((rows, d_t), jnp.float32),
            pltpu.SemaphoreType.DMA((2, 2)),
            pltpu.SemaphoreType.DMA,
            pltpu.SemaphoreType.DMA,
            pltpu.SemaphoreType.DMA((2,)),
            pltpu.SemaphoreType.DMA((2,)),
        ],
        compiler_params=pltpu.CompilerParams(collective_id=0, has_side_effects=True, vmem_limit_bytes=VMEM_LIMIT),
        cost_estimate=pl.CostEstimate(flops=8 * n_layers * rows * d_t * d_ff, bytes_accessed=4 * n_layers * d_t * d_ff,
                                      transcendentals=2 * n_layers * rows * d_ff),
        name="teacher",
    )(x, gain, w_up, w_down)


def after(value, *earlier):
    return lax.optimization_barrier((value, *earlier))[0]


def solution(mesh):
    dp_size = mesh.shape['dp']
    tp_size = mesh.shape['tp']
    swap = [(0, 1), (1, 0)]

    def local_step(x_teach, x_stud, w_up_t, w_down_t, gain_t, head_t, w_up_s, w_down_s, gain_s, proj_s, head_s):
        dp_idx = lax.axis_index('dp')
        core = lax.axis_index('tp')
        n_seq, seq_len, d_s = x_stud.shape
        d_t = x_teach.shape[-1]
        local_tok = n_seq * seq_len
        group_tok = local_tok * tp_size
        n_tokens = group_tok * dp_size
        half_cols = head_t.shape[1]
        vocab = head_s.shape[1]
        feat_coef = 1.0 / (n_tokens * d_t)
        kl_coef = 1.0 / n_tokens
        w_up, w_down, gain, proj = w_up_s[0], w_down_s[0], gain_s[0], proj_s[0]
        both = ('dp', 'tp')

        x_all = lax.all_gather(x_stud.reshape(local_tok, d_s), both, axis=0, tiled=True)
        norm_all, _ = rms_parts(x_all)
        n_all = (norm_all * gain).astype(jnp.bfloat16)

        norm_cur, _ = rms_parts(x_stud.reshape(local_tok, d_s))
        normed = (norm_cur * gain).astype(jnp.bfloat16)
        hidden_s = gelu_tanh(mat_mul('sd,df->sf', normed, w_up)).astype(jnp.bfloat16)
        residual = x_stud.reshape(local_tok, d_s).astype(jnp.float32) + mat_mul('sf,fd->sd', hidden_s, w_down)
        norm_next, inv_next = rms_parts(residual)
        proj_in = norm_next.astype(jnp.bfloat16)
        proj_out = mat_mul('sd,de->se', proj_in, proj)
        rs_flat = lax.all_gather(proj_in, both, axis=0, tiled=True)
        rs_all = rs_flat.reshape(dp_size, group_tok, d_s)
        rst_all = jnp.swapaxes(rs_all, 1, 2)
        rs_grp = lax.dynamic_index_in_dim(rs_all, dp_idx, 0, keepdims=False)

        hts = head_t.T

        f_half = w_up.shape[1] // tp_size
        up_half = lax.dynamic_slice_in_dim(w_up, core * f_half, f_half, axis=1)
        down_half = lax.dynamic_slice_in_dim(w_down, core * f_half, f_half, axis=0)
        pre_half = mat_mul('sd,df->sf', n_all, up_half)
        act_half = gelu_tanh(pre_half).astype(jnp.bfloat16)

        n_seq_t, half_seq, _ = x_teach.shape
        hidden, ht_pair = teacher(x_teach.reshape(-1, d_t), gain_t, w_up_t, w_down_t)
        feature = lax.all_to_all(hidden.reshape(n_seq_t, half_seq, d_t), 'tp', 0, 1, tiled=True)
        ht_grp = jnp.swapaxes(ht_pair.reshape(tp_size, n_seq_t, half_seq, d_t), 0, 1).reshape(group_tok, d_t)
        ht_all = lax.all_gather(ht_grp, 'dp')

        meta0 = jnp.stack([core, dp_idx, jnp.int32(0)]).astype(jnp.int32)
        zt, zs, stats = head_stats(meta0, ht_grp, rs_grp, hts, head_s, half_cols)
        stats_all = lax.all_gather(stats[:, :8].T, both).reshape(dp_size, tp_size, 8, group_tok)
        top_t, sum_t, sum_a, top_s, sum_s = [stats_all[:, :, j, :] for j in range(5)]
        max_t = jnp.max(top_t, axis=1)
        max_s = jnp.max(top_s, axis=1)
        scale_t = jnp.exp(top_t - max_t[:, None])
        all_t = jnp.sum(sum_t * scale_t, axis=1)
        all_a = jnp.sum(sum_a * scale_t, axis=1)
        all_s = jnp.sum(sum_s * jnp.exp(top_s - max_s[:, None]), axis=1)
        lse_t = max_t + jnp.log(all_t)
        lse_s = max_s + jnp.log(all_s)
        kl_total = jnp.sum(all_a / all_t - lse_t + lse_s)
        lse_t = lse_t[..., None]
        lse_s = lse_s[..., None]

        def blocks(base, count, lse, *arrays):
            meta = jnp.stack([core, dp_idx, base]).astype(jnp.int32)
            return head_grad_blocks(count, meta, ht_all, rs_all, rst_all, lse, lse_s, hts, head_s, zt, zs,
                                    half_cols, kl_coef, *arrays)

        own_parts = []
        base, lse_o = dp_idx * N_OWN, lse_t
        for count in OWN_SPLIT:
            own_parts.append(blocks(base, count, lse_o)[0])
            base = base + count
            lse_o = after(lse_t, own_parts[-1])
        shared = []
        for part in own_parts:
            shared.append(lax.all_gather(part, 'dp'))

        lse_own_t = lax.dynamic_index_in_dim(lse_o, dp_idx, 0, keepdims=False)
        lse_own_s = lax.dynamic_index_in_dim(lse_s, dp_idx, 0, keepdims=False)
        full_in_grad = head_input_grad(meta0, lse_own_t, lse_own_s, zt, zs, head_s, kl_coef)
        give = lax.dynamic_slice_in_dim(full_in_grad, (1 - core) * local_tok, local_tok, axis=0)
        keep = lax.dynamic_slice_in_dim(full_in_grad, core * local_tok, local_tok, axis=0)
        head_in_grad = keep + lax.ppermute(give, 'tp', swap)

        feat_err = proj_out - feature.reshape(local_tok, d_t)
        err_total = jnp.sum(feat_err * feat_err)
        err_grad = (2.0 * feat_coef * feat_err).astype(jnp.bfloat16)
        out_grad = mat_mul('se,de->sd', err_grad, proj)
        resid_grad = rms_back(norm_next, inv_next, out_grad + head_in_grad)
        resid_all = lax.all_gather(resid_grad.astype(jnp.bfloat16), both, axis=0, tiled=True)
        err_all = lax.all_gather(err_grad, both, axis=0, tiled=True)

        lse_r = after(lse_t, full_in_grad)
        own, partner = [], []

        def exchange(part):
            partner.append(lax.ppermute(part, 'tp', swap))
            own.append(part)

        for part in shared:
            exchange(part)
        base = jnp.int32(N_SHARED)
        full = None
        for part_idx, count in enumerate(RED_SPLIT):
            last = part_idx == len(RED_SPLIT) - 1
            arrays = ([own[0], own[0], own[2], own[3]], [partner[0], partner[0], partner[2], own[3]]) if last else ()
            part, *rest = blocks(base, count, lse_r, *arrays)
            full = rest[0] if rest else None
            exchange(part)
            base = base + count
            lse_r = after(lse_t, part)

        resid_all = after(resid_all, own[-1])
        act_grad = mat_mul('sd,fd->sf', resid_all, down_half)
        pre_grad = gelu_back(pre_half, act_grad).astype(jnp.bfloat16)
        up_part = mat_mul('sd,sf->df', n_all, pre_grad)
        down_part = mat_mul('sf,sd->fd', act_half, resid_all)
        e_half = d_t // tp_size
        proj_part = mat_mul('sd,se->de', rs_flat, lax.dynamic_slice_in_dim(err_all, core * e_half, e_half, axis=1))
        pre_own = lax.dynamic_slice_in_dim(pre_grad, dp_idx * group_tok, group_tok, axis=0)
        norm_own = lax.dynamic_slice_in_dim(norm_all, dp_idx * group_tok, group_tok, axis=0)
        gain_part = jnp.sum(mat_mul('sf,df->sd', pre_own, up_half) * norm_own, axis=0)

        grad_up = lax.all_gather(up_part, 'tp', axis=1, tiled=True)[None]
        grad_down = lax.all_gather(down_part, 'tp', axis=0, tiled=True)[None]
        grad_proj = lax.all_gather(proj_part, 'tp', axis=1, tiled=True)[None]
        small = jnp.concatenate([gain_part, err_total[None], jnp.zeros((1023 - d_s,), jnp.float32)]).reshape(8, 128)
        small = jnp.sum(lax.all_gather(small, both), axis=0).reshape(1024)
        grad_gain, err_sum = small[:d_s], small[d_s]
        loss = feat_coef * err_sum + kl_coef * kl_total
        head_grad = assemble(meta0, own, partner, full, vocab)
        return loss, grad_up, grad_down, grad_gain[None], grad_proj, head_grad

    in_specs = (P('dp', 'tp', None), P(('dp', 'tp'), None, None), P(None, None, 'tp'), P(None, 'tp', None),
                P(), P(None, 'tp'), P(), P(), P(), P(), P())
    out_specs = (P(), P(), P(), P(), P(), P())

    return jax.shard_map(local_step, mesh=mesh, in_specs=in_specs, out_specs=out_specs, check_vma=False)
```
